32 devices in a mesh: groups: 2 (over x), tensor: 16 (over z, y, core).
Axes of the slice: x: 2, y: 2, z: 4, core: 2. Of those that a mesh axis runs over, the one named last changes fastest.
Arguments:
- span_rows: bfloat16 [32, 8192], P(('groups', 'tensor')), parts along dimension 0, may hold values from -6 to 6
- decode_rows: bfloat16 [2, 32, 8192], P(None, ('groups', 'tensor')), parts along dimension 1, may hold values from -6 to 6
- norm_gain: bfloat16 [8192], replicated, may hold values from 0.099609375 to 1.8984375
- w_query: bfloat16 [8192, 8192], P(None, 'tensor'), may hold values from -0.0625 to 0.0625
- w_keyval: bfloat16 [8192, 2048], P(None, 'tensor'), may hold values from -0.0625 to 0.0625
- prefix_keys: bfloat16 [8192, 1024], P(('groups', 'tensor')), parts along dimension 0, may hold values from -304 to 304
- prefix_values: bfloat16 [8192, 1024], P(('groups', 'tensor')), parts along dimension 0, may hold values from -6 to 6
- span_offset: int32 [2], P('groups'), parts along dimension 0, may hold values from 2048 to 4096
- pool_keys: bfloat16 [1024, 16, 1024], P(('groups', 'tensor')), parts along dimension 0, may hold values from -304 to 304
- pool_values: bfloat16 [1024, 16, 1024], P(('groups', 'tensor')), parts along dimension 0, may hold values from -6 to 6
- row_blocks: int32 [32, 32], P('groups'), parts along dimension 0, may hold values from 0 to 511, as said below
- context_lens: int32 [32], P('groups'), parts along dimension 0, may hold values from 1 to 512, 4096 in all
Outputs:
- span_attended: bfloat16 [32, 8192], P(('groups', 'tensor')), parts along dimension 0
- decode_attended: bfloat16 [2, 32, 8192], P(None, ('groups', 'tensor')), parts along dimension 1
- span_cache: bfloat16 [32, 2048], P(('groups', 'tensor')), parts along dimension 0
The draws below stay inside these ranges and needn't reach their ends.
There are 2 independent parts, one for each index of `groups`. The reference program is written for one: setup_inputs(seed, part) draws one part's arguments, and reference() takes and returns one part's arrays. A program takes and returns all parts, laid end to end along the dimension named above; an argument that names none is the same for every part. Nothing has to cross between parts.
Inputs may be any that keep to these rules, and one draw needn't show every extreme that they name: Prefix slots from span_offset on are unused. `row_blocks`: every cache block belongs to exactly one decode row; entry k of a row holds its positions k * 16 to k * 16 + 15. `context_lens`: some row has exactly 512 cached tokens.
All inputs are finite; a program needn't handle non-finite values.
Results may differ from the reference program's by a relative error of at most 0.0065.
The reference program's roundings to bfloat16 on the way count: a program that leaves them out, or rounds other values in their place, can miss the bound.
Values may be sent and summed in bfloat16 or wider, within the bound.
No kernel may reach another device: no remote copies, remote signals or barrier semaphores. Data moves between devices by JAX's collectives and lax.ppermute only.
A program may use at most 128 MiB of HBM per device.

```python
import math
import jax
import jax.numpy as jnp
import numpy as np
from jax import lax

D = 8192
H = 64
KVH = 8
HD = 128
PAGE = 16
STEPS = 2
SPAN = 16
ROWS = 16
PREFIX = 4096
BLOCKS = 512
BLK_ROW = 32


def block_order(key):
    return jax.random.permutation(jax.random.fold_in(key, 11), BLOCKS).astype(jnp.int32).reshape(ROWS, BLK_ROW)


def draw_row_blocks(key, part):
    return block_order(key)


def draw_prefix_keys(key, part):
    key_width = KVH * HD
    drawn = jnp.clip(jax.random.normal(jax.random.fold_in(key, 5), (PREFIX, key_width), jnp.float32), -6.0, 6.0)
    return drawn.astype(jnp.bfloat16)


def draw_pool_keys(key, part):
    key_width = KVH * HD
    drawn = jnp.clip(jax.random.normal(jax.random.fold_in(key, 19), (BLOCKS, PAGE, key_width), jnp.float32), -6.0, 6.0)
    return drawn.astype(jnp.bfloat16)


def block_levels(rng, dims, cuts, smallest, largest):
    gain, own = 1.0, jax.random.fold_in(rng, 6)
    for position, parts in cuts:
        draws = jnp.exp(jax.random.uniform(jax.random.fold_in(own, position), (parts,), jnp.float32, smallest / len(cuts), largest / len(cuts)))
        gain = gain * jnp.repeat(draws, dims[position] // parts).reshape([-1 if axis == position else 1 for axis in range(len(dims))])
    return gain


def split_up(number_of, total, most, lean):
    weights = [(1 << 20) // math.isqrt(grade ** lean) + 1 for grade in range(2, number_of + 1)]
    surplus, counts = total - most - (number_of - 1), [1] * (number_of - 1)
    while surplus > 0:
        free = [i for i in range(number_of - 1) if counts[i] < most]
        whole, budget = sum([weights[i] for i in free]), surplus
        for i in free:
            more = min(most - counts[i], max(1, budget * weights[i] // whole), surplus)
            counts[i] = counts[i] + more
            surplus = surplus - more
    return np.array([most] + counts)


def ragged(rng, amount, total, bound, slope):
    if amount == 2:
        one = jax.random.randint(rng, (), max(1, total - bound), min(bound, total - 1) + 1)
        return jnp.stack([one, total - one])
    sizes = jnp.asarray(split_up(amount, total, bound, slope), jnp.int32)
    twos = (amount - 1) // 2
    source_of, taker = sizes[1:1 + 2 * twos:2], sizes[2:2 + 2 * twos:2]
    margin = jnp.minimum(source_of - 1, bound - taker)
    shifted = jax.random.randint(jax.random.fold_in(rng, 1), (twos,), 0, 1 << 20) % (margin + 1)
    sizes = sizes.at[1:1 + 2 * twos:2].set(source_of - shifted).at[2:2 + 2 * twos:2].set(taker + shifted)
    return sizes[jax.random.permutation(jax.random.fold_in(rng, 2), amount)]


def noise(stream_key, dims, spread, reach, split=(), held_as=jnp.bfloat16):
    gain = block_levels(stream_key, dims, split, -0.22, 0.18) if split else 1.0
    entries = jax.random.normal(stream_key, dims, jnp.float32) * spread * gain
    return jnp.minimum(jnp.maximum(entries, -reach), reach).astype(held_as)


def setup_inputs(seed: int = 0, part: int = 0) -> dict:
    keys = jax.random.split(jax.random.key(seed), 13)
    own_keys = jax.random.split(jax.random.fold_in(keys[12], part), 13)
    span_rows = noise(own_keys[0], (SPAN, D), 1.0, 6.0, ((0, 16),))
    decode_rows = noise(own_keys[1], (STEPS, ROWS, D), 1.0, 6.0, ((1, 16),))
    norm_gain = jnp.clip(1.0 + 0.18 * jax.random.normal(keys[2], (D,), jnp.float32), 0.099609375, 1.8984375).astype(jnp.bfloat16)
    w_query = noise(keys[3], (D, D), D ** -0.5, 0.0625, ((1, 16),))
    w_keyval = noise(keys[4], (D, 2 * KVH * HD), D ** -0.5, 0.0625, ((1, 16),))
    prefix_keys = draw_prefix_keys(jax.random.fold_in(jax.random.fold_in(keys[12], part), 71), part)
    prefix_values = noise(own_keys[6], (PREFIX, KVH * HD), 1.0, 6.0, ((0, 16),))
    span_offset = jax.random.randint(own_keys[7], (1,), PREFIX // 2, PREFIX + 1).astype(jnp.int32)
    pool_keys = draw_pool_keys(jax.random.fold_in(jax.random.fold_in(keys[12], part), 71), part)
    pool_values = noise(own_keys[9], (BLOCKS, PAGE, KVH * HD), 1.0, 6.0, ((0, 16),))
    row_blocks = draw_row_blocks(jax.random.fold_in(jax.random.fold_in(keys[12], part), 71), part)
    context_lens = ragged(own_keys[11], ROWS, ROWS * BLK_ROW * PAGE // 2, BLK_ROW * PAGE, 2).astype(jnp.int32)
    return dict(span_rows=span_rows, decode_rows=decode_rows, norm_gain=norm_gain, w_query=w_query, w_keyval=w_keyval, prefix_keys=prefix_keys, prefix_values=prefix_values, span_offset=span_offset, pool_keys=pool_keys, pool_values=pool_values, row_blocks=row_blocks, context_lens=context_lens)


epsilon = 1e-05
neg_fill = -1e+30
rotation_bits = 20

def normalize(row_block, gain_vector):
    widened = row_block.astype(jnp.float32)
    mean_square = lax.optimization_barrier(jnp.mean(widened * widened, axis=-1, keepdims=True))
    return (widened * lax.rsqrt(mean_square + epsilon) * gain_vector.astype(jnp.float32)).astype(jnp.bfloat16)

def llama_frequencies(half_width):
    exponents = np.arange(half_width) / (1.0 * half_width)
    inverse = 1.0 / 500000.0 ** exponents
    wavelen = 2.0 * np.pi / inverse
    scaled = np.where(wavelen > 8192.0, inverse / 8.0, inverse)
    smooth = (8192.0 / wavelen - 1.0) / 3.0
    blended = (1.0 - smooth) * inverse / 8.0 + smooth * inverse
    middle = (wavelen >= 2048.0) & (wavelen <= 8192.0)
    return np.where(middle, blended, scaled)

def rotation_tables(half_width):
    frequencies = llama_frequencies(half_width)
    powers = 2.0 ** np.arange(rotation_bits)
    angles = powers[:, None] * frequencies[None, :]
    return (jnp.asarray(np.cos(angles), jnp.float32), jnp.asarray(np.sin(angles), jnp.float32))

def rotate(projected, positions, head_count):
    row_count = projected.shape[0]
    half_width = HD // 2
    cos_table, sin_table = rotation_tables(half_width)
    cos_part = jnp.ones((row_count, half_width), jnp.float32)
    sin_part = jnp.zeros((row_count, half_width), jnp.float32)
    for bit_index in range(rotation_bits):
        chosen = (positions >> bit_index & 1).astype(jnp.float32)[:, None]
        step_cos = 1.0 + chosen * (cos_table[bit_index] - 1.0)
        step_sin = chosen * sin_table[bit_index]
        cos_part, sin_part = (cos_part * step_cos - sin_part * step_sin, sin_part * step_cos + cos_part * step_sin)
    shaped = projected.astype(jnp.float32).reshape(row_count, head_count, HD)
    first_half = shaped[..., :half_width]
    second_half = shaped[..., half_width:]
    cos_part = cos_part[:, None, :]
    sin_part = sin_part[:, None, :]
    turned = jnp.concatenate([first_half * cos_part - second_half * sin_part, second_half * cos_part + first_half * sin_part], axis=-1)
    return turned.reshape(row_count, head_count * HD).astype(jnp.bfloat16)

def soft_attend(queries, key_rows, value_rows, allowed, score_scale, form_scores, form_values):
    scores = jnp.einsum(form_scores, queries, key_rows) * score_scale
    scores = jnp.where(allowed, scores, neg_fill)
    row_max = lax.optimization_barrier(jnp.max(scores, axis=-1, keepdims=True))
    weights = jnp.where(allowed, jnp.exp(scores - row_max), 0.0)
    weight_sum = lax.optimization_barrier(jnp.sum(weights, axis=-1))
    rounded = lax.optimization_barrier(weights.astype(jnp.bfloat16)).astype(jnp.float32)
    numerator = jnp.einsum(form_values, rounded, value_rows)
    return (numerator / weight_sum[..., None]).astype(jnp.bfloat16)

def reference(span_rows, decode_rows, norm_gain, w_query, w_keyval, prefix_keys, prefix_values, span_offset, pool_keys, pool_values, row_blocks, context_lens):
    group_size = H // KVH
    kv_width = KVH * HD
    score_scale = 1.0 / math.sqrt(HD)
    offset = span_offset[0]

    def project(normed):
        queries = jnp.dot(normed, w_query, preferred_element_type=jnp.float32).astype(jnp.bfloat16)
        keyval = jnp.dot(normed, w_keyval, preferred_element_type=jnp.float32).astype(jnp.bfloat16)
        return (queries, keyval)
    span_queries, span_keyval = project(normalize(span_rows, norm_gain))
    decode_queries, decode_keyval = project(normalize(decode_rows.reshape(STEPS * ROWS, D), norm_gain))
    span_positions = offset + jnp.arange(SPAN, dtype=jnp.int32)
    decode_positions = (context_lens[None, :] + jnp.arange(STEPS, dtype=jnp.int32)[:, None]).reshape(-1)
    span_queries = rotate(span_queries, span_positions, H)
    span_keys = rotate(span_keyval[:, :kv_width], span_positions, KVH)
    span_values = span_keyval[:, kv_width:]
    decode_queries = rotate(decode_queries, decode_positions, H).reshape(STEPS, ROWS, D)
    decode_keys = rotate(decode_keyval[:, :kv_width], decode_positions, KVH).reshape(STEPS, ROWS, kv_width)
    decode_values = decode_keyval[:, kv_width:].reshape(STEPS, ROWS, kv_width)
    span_cache = jnp.concatenate([span_keys, span_values], axis=1)
    key_count = PREFIX + SPAN
    keys_by_head = jnp.concatenate([prefix_keys, span_keys], axis=0).reshape(key_count, KVH, HD).transpose(1, 0, 2)
    values_by_head = jnp.concatenate([prefix_values, span_values], axis=0).reshape(key_count, KVH, HD).transpose(1, 0, 2)
    query_block = min(SPAN, 16)
    block_count = SPAN // query_block
    queries_by_head = span_queries.reshape(SPAN, KVH, group_size, HD).transpose(1, 0, 2, 3)
    key_index = jnp.arange(key_count, dtype=jnp.int32)
    query_index = jnp.arange(SPAN, dtype=jnp.int32).reshape(block_count, query_block)

    def per_head(packed):
        head_queries, head_keys, head_values = packed
        keys_wide = head_keys.astype(jnp.float32)
        values_wide = head_values.astype(jnp.float32)

        def per_block(inner):
            block_queries, block_index = inner
            allowed = jnp.where(key_index[None, :] < PREFIX, key_index[None, :] < offset, key_index[None, :] - PREFIX <= block_index[:, None])
            return soft_attend(block_queries.astype(jnp.float32), keys_wide, values_wide, allowed[:, None, :], score_scale, 'iqd,kd->iqk', 'iqk,kd->iqd')
        return lax.map(per_block, (head_queries.reshape(block_count, query_block, group_size, HD), query_index))
    results = lax.map(per_head, (queries_by_head, keys_by_head, values_by_head))
    span_attended = results.reshape(KVH, SPAN, group_size, HD).transpose(1, 0, 2, 3).reshape(SPAN, D)
    context = BLK_ROW * PAGE
    seen_index = jnp.arange(context + STEPS, dtype=jnp.int32)
    step_index = jnp.arange(STEPS, dtype=jnp.int32)

    def per_row(packed):
        blocks, length, row_queries, new_keys, new_values = packed
        row_keys = jnp.take(pool_keys, blocks, axis=0).reshape(context, KVH, HD)
        row_values = jnp.take(pool_values, blocks, axis=0).reshape(context, KVH, HD)
        row_keys = jnp.concatenate([row_keys, new_keys.reshape(STEPS, KVH, HD)], axis=0).astype(jnp.float32)
        row_values = jnp.concatenate([row_values, new_values.reshape(STEPS, KVH, HD)], axis=0).astype(jnp.float32)
        allowed = jnp.where(seen_index[None, :] < context, seen_index[None, :] < length, seen_index[None, :] - context <= step_index[:, None])
        shaped = row_queries.reshape(STEPS, KVH, group_size, HD).astype(jnp.float32)
        attended = soft_attend(shaped, row_keys, row_values, allowed[:, None, None, :], score_scale, 'sgqd,kgd->sgqk', 'sgqk,kgd->sgqd')
        return attended.reshape(STEPS, D)
    decoded = lax.map(per_row, (row_blocks, context_lens, decode_queries.transpose(1, 0, 2), decode_keys.transpose(1, 0, 2), decode_values.transpose(1, 0, 2)))
    decode_attended = decoded.transpose(1, 0, 2)
    return (span_attended, decode_attended, span_cache)
```

```python
import math

import jax
import jax.numpy as jnp
import numpy as np
from jax import lax
from jax.experimental import pallas as pl
from jax.experimental.pallas import tpu as pltpu
from jax.sharding import PartitionSpec as P

D = 8192
H = 64
KVH = 8
HD = 128
PAGE = 16
STEPS = 2
BLK_ROW = 32


epsilon = 1e-05
neg_fill = -1e30
rotation_bits = 20


def normalize(row_block, gain_vector):
    widened = row_block.astype(jnp.float32)
    mean_square = jnp.mean(widened * widened, axis=-1, keepdims=True)
    return (widened * lax.rsqrt(mean_square + epsilon) * gain_vector.astype(jnp.float32)).astype(
        jnp.bfloat16
    )


def llama_frequencies(half_width):
    exponents = np.arange(half_width) / (1.0 * half_width)
    inverse = 1.0 / 500000.0**exponents
    wavelen = 2.0 * np.pi / inverse
    scaled = np.where(wavelen > 8192.0, inverse / 8.0, inverse)
    smooth = (8192.0 / wavelen - 1.0) / 3.0
    blended = (1.0 - smooth) * inverse / 8.0 + smooth * inverse
    middle = (wavelen >= 2048.0) & (wavelen <= 8192.0)
    return np.where(middle, blended, scaled)


def rotation_tables(half_width):
    frequencies = llama_frequencies(half_width)
    powers = 2.0 ** np.arange(rotation_bits)
    angles = powers[:, None] * frequencies[None, :]
    return (jnp.asarray(np.cos(angles), jnp.float32), jnp.asarray(np.sin(angles), jnp.float32))


def rotate(projected, positions, head_count):
    row_count = projected.shape[0]
    half_width = HD // 2
    cos_table, sin_table = rotation_tables(half_width)
    cos_part = jnp.ones((row_count, half_width), jnp.float32)
    sin_part = jnp.zeros((row_count, half_width), jnp.float32)
    for bit_index in range(rotation_bits):
        chosen = (positions >> bit_index & 1).astype(jnp.float32)[:, None]
        step_cos = 1.0 + chosen * (cos_table[bit_index] - 1.0)
        step_sin = chosen * sin_table[bit_index]
        cos_part, sin_part = (
            cos_part * step_cos - sin_part * step_sin,
            sin_part * step_cos + cos_part * step_sin,
        )
    shaped = projected.astype(jnp.float32).reshape(row_count, head_count, HD)
    first_half = shaped[..., :half_width]
    second_half = shaped[..., half_width:]
    cos_part = cos_part[:, None, :]
    sin_part = sin_part[:, None, :]
    turned = jnp.concatenate(
        [
            first_half * cos_part - second_half * sin_part,
            second_half * cos_part + first_half * sin_part,
        ],
        axis=-1,
    )
    return turned.reshape(row_count, head_count * HD).astype(jnp.bfloat16)


def generic_shards(
    span_rows,
    decode_rows,
    norm_gain,
    w_query,
    w_keyval,
    prefix_keys,
    prefix_values,
    span_offset,
    pool_keys,
    pool_values,
    row_blocks,
    context_lens,
):
    devices = lax.axis_size("tensor")
    my_rank = lax.axis_index("tensor")
    span_dev = span_rows.shape[0]
    rows_dev = decode_rows.shape[1]
    local_count = span_dev + STEPS * rows_dev
    group_size = H // KVH
    kv_width = KVH * HD
    score_scale = 1.0 / math.sqrt(HD)
    offset = span_offset[0]
    row_total = context_lens.shape[0]
    span_total = span_dev * devices
    query_cols = w_query.shape[1]
    local_rows = jnp.concatenate([span_rows, decode_rows.reshape(STEPS * rows_dev, D)], axis=0)
    normed = normalize(local_rows, norm_gain)
    shard_rows = lax.all_gather(normed, "tensor", axis=0, tiled=True)
    queries = jnp.dot(shard_rows, w_query, preferred_element_type=jnp.float32)
    keyval = jnp.dot(shard_rows, w_keyval, preferred_element_type=jnp.float32)
    projected = jnp.concatenate([queries, keyval], axis=1).astype(jnp.bfloat16)
    query_part = projected[:, :query_cols]
    keyval_part = projected[:, query_cols:]
    device_ids = jnp.arange(devices, dtype=jnp.int32)[:, None]
    local_ids = jnp.arange(local_count, dtype=jnp.int32)[None, :]
    span_positions = offset + device_ids * span_dev + local_ids
    decode_local = jnp.maximum(local_ids - span_dev, 0)
    owner_rows = device_ids * rows_dev + decode_local % rows_dev
    decode_positions = jnp.take(context_lens, owner_rows) + decode_local // rows_dev
    positions = jnp.where(local_ids < span_dev, span_positions, decode_positions)
    my_positions = lax.dynamic_index_in_dim(positions, my_rank, 0, keepdims=False)
    queries_full, keyval_full = (
        lax.all_gather(query_part, "tensor", axis=1, tiled=True),
        lax.all_gather(keyval_part, "tensor", axis=1, tiled=True),
    )
    keyval_own = lax.dynamic_slice_in_dim(keyval_full, my_rank * local_count, local_count, 0)
    queries_rot = rotate(queries_full, positions.reshape(-1), H).reshape(devices, local_count, D)
    keys_own = rotate(keyval_own[:, :kv_width], my_positions, KVH)
    values_own = keyval_own[:, kv_width:]
    span_cache = jnp.concatenate([keys_own[:span_dev], values_own[:span_dev]], axis=1)
    span_queries = queries_rot[:, :span_dev].reshape(span_total, KVH, group_size, HD)
    local_keys = jnp.concatenate([prefix_keys, keys_own[:span_dev]], axis=0).reshape(-1, KVH, HD)
    local_values = jnp.concatenate([prefix_values, values_own[:span_dev]], axis=0).reshape(
        -1, KVH, HD
    )
    prefix_dev = prefix_keys.shape[0]
    slot_ids = jnp.arange(prefix_dev + span_dev, dtype=jnp.int32)
    prefix_pos = my_rank * prefix_dev + slot_ids
    span_token = my_rank * span_dev + slot_ids - prefix_dev
    query_ids = jnp.arange(span_total, dtype=jnp.int32)[:, None]
    allowed = jnp.where(
        slot_ids[None, :] < prefix_dev,
        (prefix_pos < offset)[None, :],
        span_token[None, :] <= query_ids,
    )
    span_scores = (
        jnp.einsum("igqd,kgd->igqk", span_queries, local_keys, preferred_element_type=jnp.float32)
        * score_scale
    )
    span_scores = jnp.where(allowed[:, None, None, :], span_scores, neg_fill)
    span_peak = jnp.max(span_scores, axis=-1)
    block_dev = pool_keys.shape[0]
    block_ids = my_rank * block_dev + jnp.arange(block_dev, dtype=jnp.int32)
    flat_map = row_blocks.reshape(-1)
    entry_ids = jnp.arange(flat_map.shape[0], dtype=jnp.int32)
    found_at = jnp.sum(
        jnp.where(flat_map[None, :] == block_ids[:, None], entry_ids[None, :], 0), axis=1
    )
    block_rows = found_at // BLK_ROW
    block_slots = found_at % BLK_ROW
    token_pos = block_slots[:, None] * PAGE + jnp.arange(PAGE, dtype=jnp.int32)[None, :]
    live_tokens = token_pos < jnp.take(context_lens, block_rows)[:, None]
    decode_queries = (
        queries_rot[:, span_dev:]
        .reshape(devices, STEPS, rows_dev, D)
        .transpose(0, 2, 1, 3)
        .reshape(row_total, STEPS, D)
    )
    block_queries = jnp.take(decode_queries, block_rows, axis=0).reshape(
        block_dev, STEPS, KVH, group_size, HD
    )
    block_keys = pool_keys.reshape(block_dev, PAGE, KVH, HD)
    block_scores = (
        jnp.einsum(
            "bsgqd,bugd->bsgqu", block_queries, block_keys, preferred_element_type=jnp.float32
        )
        * score_scale
    )
    block_scores = jnp.where(live_tokens[:, None, None, None, :], block_scores, neg_fill)
    block_peak = jnp.max(block_scores, axis=-1)
    member = block_rows[:, None] == jnp.arange(row_total, dtype=jnp.int32)[None, :]
    row_peak = jnp.max(
        jnp.where(member[:, :, None, None, None], block_peak[:, None], neg_fill), axis=0
    )
    own_start = my_rank * rows_dev
    own_queries = lax.dynamic_slice_in_dim(decode_queries, own_start, rows_dev, 0).reshape(
        rows_dev, STEPS, KVH, group_size, HD
    )
    new_keys = keys_own[span_dev:].reshape(STEPS, rows_dev, KVH, HD)
    new_values = values_own[span_dev:].reshape(STEPS, rows_dev, KVH, HD)
    new_scores = (
        jnp.einsum("rsgqd,trgd->rsgqt", own_queries, new_keys, preferred_element_type=jnp.float32)
        * score_scale
    )
    step_ids = jnp.arange(STEPS, dtype=jnp.int32)
    causal = (step_ids[None, :] <= step_ids[:, None])[None, :, None, None, :]
    new_scores = jnp.where(causal, new_scores, neg_fill)
    own_peak = lax.dynamic_slice_in_dim(row_peak, own_start, rows_dev, 0)
    row_peak = lax.dynamic_update_slice_in_dim(
        row_peak, jnp.maximum(own_peak, jnp.max(new_scores, axis=-1)), own_start, 0
    )
    span_top, row_top = lax.pmax((span_peak, row_peak), "tensor")
    span_weights = jnp.where(
        allowed[:, None, None, :], jnp.exp(span_scores - span_top[..., None]), 0.0
    )
    span_den = jnp.sum(span_weights, axis=-1).reshape(span_total, H)
    span_num = jnp.einsum(
        "igqk,kgd->igqd",
        span_weights.astype(jnp.bfloat16),
        local_values,
        preferred_element_type=jnp.float32,
    ).reshape(span_total, D)
    block_top = jnp.take(row_top, block_rows, axis=0)
    block_weights = jnp.where(
        live_tokens[:, None, None, None, :], jnp.exp(block_scores - block_top[..., None]), 0.0
    )
    block_den = jnp.sum(block_weights, axis=-1).reshape(block_dev, STEPS * H)
    block_values = pool_values.reshape(block_dev, PAGE, KVH, HD)
    block_num = jnp.einsum(
        "bsgqu,bugd->bsgqd",
        block_weights.astype(jnp.bfloat16),
        block_values,
        preferred_element_type=jnp.float32,
    ).reshape(block_dev, STEPS * D)
    member_wide = member.astype(jnp.float32).T
    row_num = jnp.dot(member_wide, block_num, precision=lax.Precision.HIGHEST)
    row_den = jnp.dot(member_wide, block_den, precision=lax.Precision.HIGHEST)
    own_top = lax.dynamic_slice_in_dim(row_top, own_start, rows_dev, 0)
    new_weights = jnp.where(causal, jnp.exp(new_scores - own_top[..., None]), 0.0)
    new_den = jnp.sum(new_weights, axis=-1).reshape(rows_dev, STEPS * H)
    new_num = jnp.einsum(
        "rsgqt,trgd->rsgqd",
        new_weights.astype(jnp.bfloat16),
        new_values,
        preferred_element_type=jnp.float32,
    ).reshape(rows_dev, STEPS * D)
    row_num = lax.dynamic_update_slice_in_dim(
        row_num, lax.dynamic_slice_in_dim(row_num, own_start, rows_dev, 0) + new_num, own_start, 0
    )
    row_den = lax.dynamic_update_slice_in_dim(
        row_den, lax.dynamic_slice_in_dim(row_den, own_start, rows_dev, 0) + new_den, own_start, 0
    )
    row_num, row_den = (row_num, row_den)
    span_sum, span_weight, row_sum, row_weight = (
        lax.psum_scatter(span_num, "tensor", scatter_dimension=0, tiled=True),
        lax.psum_scatter(span_den, "tensor", scatter_dimension=0, tiled=True),
        lax.psum_scatter(row_num, "tensor", scatter_dimension=0, tiled=True),
        lax.psum_scatter(row_den, "tensor", scatter_dimension=0, tiled=True),
    )
    span_attended = (
        (span_sum.reshape(span_dev, H, HD) / span_weight.reshape(span_dev, H, 1))
        .reshape(span_dev, D)
        .astype(jnp.bfloat16)
    )
    decode_attended = (
        row_sum.reshape(rows_dev, STEPS, H, HD) / row_weight.reshape(rows_dev, STEPS, H, 1)
    ).astype(jnp.bfloat16)
    decode_attended = decode_attended.reshape(rows_dev, STEPS, D).transpose(1, 0, 2)
    return (span_attended, decode_attended, span_cache)


SEGMENTS = 8
TYPES = STEPS + 1
VMEM_LIMIT = 24 * 1024 * 1024


def vmem():
    return pl.BlockSpec(memory_space=pltpu.VMEM)


def smem():
    return pl.BlockSpec(memory_space=pltpu.SMEM)


def call(body, out_shape, in_specs, scratch=(), flops=0, moved=0, name=None):
    many = isinstance(out_shape, (list, tuple))
    return pl.pallas_call(
        body,
        out_shape=out_shape,
        in_specs=in_specs,
        out_specs=[vmem() for _ in out_shape] if many else vmem(),
        scratch_shapes=list(scratch),
        compiler_params=pltpu.CompilerParams(vmem_limit_bytes=VMEM_LIMIT),
        cost_estimate=pl.CostEstimate(flops=flops, bytes_accessed=moved, transcendentals=0),
        name=name,
    )


def norm_kernel(span_ref, decode_ref, gain_ref, out_ref, rows, gains):
    width = D // SEGMENTS
    for s in range(SEGMENTS):
        cut = slice(s * width, (s + 1) * width)
        rows[s : s + 1, :] = span_ref[:, cut].astype(jnp.float32)
        both = decode_ref[:, cut].astype(jnp.float32)
        for t in range(STEPS):
            at = (t + 1) * SEGMENTS + s
            rows[at : at + 1, :] = both[t : t + 1]
        gains[s : s + 1, :] = gain_ref[:, cut].astype(jnp.float32)
    gain = gains[...]
    for r in range(TYPES):
        x = rows[r * SEGMENTS : (r + 1) * SEGMENTS, :]
        total = jnp.sum(jnp.sum(x * x, axis=1, keepdims=True), axis=0, keepdims=True)
        y = x * lax.rsqrt(total / D + epsilon) * gain
        out_ref[r * SEGMENTS : (r + 1) * SEGMENTS, :] = y.astype(jnp.bfloat16)


def table_kernel(
    me_ref, offset_ref, lens_ref, blocks_ref, cos_tab, sin_tab,
    cos_ref, sin_ref, live_ref, seen_ref, lens_col,
):
    owners = lens_ref.shape[0]
    chips = owners // 2
    total = TYPES * owners
    row = lax.broadcasted_iota(jnp.int32, (total, HD), 0)
    kind = row // owners
    within = row % owners
    owner = (within % chips) * 2 + within // chips
    base = jnp.zeros((total, HD), jnp.int32)
    for r in range(owners):
        base = jnp.where(owner == r, lens_ref[r], base)
        lens_col[r : r + 1, :] = jnp.full((1, HD), lens_ref[r], jnp.int32)
    position = jnp.where(kind == 0, offset_ref[0] + owner, base + kind - 1)
    cos_part = jnp.ones((total, HD), jnp.float32)
    sin_part = jnp.zeros((total, HD), jnp.float32)
    for bit in range(rotation_bits):
        chosen = (lax.shift_right_logical(position, bit) & 1) == 1
        step_cos = jnp.where(chosen, cos_tab[bit : bit + 1, :], 1.0)
        step_sin = jnp.where(chosen, sin_tab[bit : bit + 1, :], 0.0)
        cos_part, sin_part = (
            cos_part * step_cos - sin_part * step_sin,
            sin_part * step_cos + cos_part * step_sin,
        )
    lane = lax.broadcasted_iota(jnp.int32, (total, HD), 1)
    cos_ref[...] = cos_part
    sin_ref[...] = jnp.where(lane < HD // 2, -sin_part, sin_part)
    tokens = live_ref.shape[1]
    blocks_dev = tokens // PAGE
    token = lax.broadcasted_iota(jnp.int32, (owners, tokens), 1)
    block = me_ref[0] * blocks_dev + token // PAGE
    place = jnp.full((owners, tokens), 1 << 30, jnp.int32)
    table = blocks_ref[...]
    for k in range(BLK_ROW):
        hit = table[:, k : k + 1] == block
        place = jnp.where(hit, k * PAGE + token % PAGE, place)
    live = jnp.where(place < lens_col[:, 0:1], 0.0, neg_fill)
    for c in range(2):
        for p in range(chips):
            o = 2 * p + c
            live_ref[c * chips + p : c * chips + p + 1, :] = live[o : o + 1]
    slots = seen_ref.shape[1]
    slot = lax.broadcasted_iota(jnp.int32, (8, slots), 1) + me_ref[0] * slots
    seen_ref[...] = jnp.where(slot < offset_ref[0], 0.0, neg_fill)


def project_kernel(
    me_ref, rows_ref, wq_ref, wkv_ref, cos_ref, sin_ref, out_ref, wide, acc
):
    step = pl.program_id(0)
    count = rows_ref.shape[0] // SEGMENTS
    cols = wq_ref.shape[1]

    @pl.when(step == 0)
    def _():
        for j in range(wide.shape[0]):
            wide[j] = rows_ref[:, j * HD : (j + 1) * HD].astype(jnp.float32)
        acc[...] = jnp.zeros_like(acc)

    left = jnp.concatenate(
        [wide[j, pl.ds(step, count, stride=SEGMENTS), :] for j in range(wide.shape[0])], axis=1
    ).astype(jnp.bfloat16)
    acc[:, :cols] += jnp.dot(left, wq_ref[...], preferred_element_type=jnp.float32)
    acc[:, cols:] += jnp.dot(left, wkv_ref[...], preferred_element_type=jnp.float32)

    @pl.when(step == SEGMENTS - 1)
    def _():
        owners = count // TYPES
        chips = owners // 2
        to = lax.broadcasted_iota(jnp.int32, (count, count), 0)
        frm = lax.broadcasted_iota(jnp.int32, (count, count), 1)
        kind = to // owners
        within = to % owners
        owner = (within % chips) * 2 + within // chips
        pick = (frm == owner * TYPES + kind).astype(jnp.bfloat16)
        rounded = acc[...].astype(jnp.bfloat16)
        placed = jnp.dot(pick, rounded, preferred_element_type=jnp.float32)
        cos = cos_ref[...]
        sin = sin_ref[...]
        is_key = me_ref[0] < KVH
        for h in range(out_ref.shape[1] // HD):
            x = placed[:, h * HD : (h + 1) * HD]
            turned = x * cos + pltpu.roll(x, HD // 2, 1) * sin
            if h * HD >= cols:
                turned = jnp.where(is_key, turned, x)
            out_ref[:, h * HD : (h + 1) * HD] = turned.astype(jnp.bfloat16)


def soften(scores, bias, values, heads):
    scale = 1.0 / math.sqrt(HD)
    rows, keys = bias.shape
    s = (scores * scale).reshape(heads, rows, keys) + bias[None]
    s = s.reshape(heads * rows, keys)
    top = jnp.max(s, axis=1, keepdims=True)
    w = jnp.exp(s - top)
    den = jnp.sum(w, axis=1, keepdims=True)
    num = jnp.dot(w.astype(jnp.bfloat16), values, preferred_element_type=jnp.float32)
    return num / den, top + jnp.log(den)


def nt_dot(a, b):
    return lax.dot_general(a, b, (((1,), (1,)), ((), ())), preferred_element_type=jnp.float32)


def split3(x):
    hi = x.astype(jnp.bfloat16)
    left = x - hi.astype(jnp.float32)
    mid = left.astype(jnp.bfloat16)
    low = (left - mid.astype(jnp.float32)).astype(jnp.bfloat16)
    return hi, mid, low


def attend_kernel(
    me_ref, q_ref, pk_ref, pv_ref, ck_ref, cv_ref, live_ref, seen_ref,
    keep_ref, send_ref, keep_log, send_log, logs,
):
    owners = live_ref.shape[0]
    chips = owners // 2
    group = H // KVH
    per_dev = group // 2
    core = me_ref[0] % 2
    first = core == 0
    live = jnp.concatenate([live_ref[...]] * STEPS, axis=0)
    seen = jnp.concatenate([seen_ref[...]] * (owners // 8), axis=0)
    lane = lax.broadcasted_iota(jnp.int32, (TYPES * owners, HD), 1)
    logs[...] = jnp.zeros_like(logs)

    def place(out, log, heads, base, kind0, kinds):
        for j in range(len(heads)):
            h = heads[j]
            at = slice(h * HD, (h + 1) * HD)
            for k in range(kinds):
                t = kind0 + k
                o0 = out[(j * kinds + k) * owners : (j * kinds + k) * owners + chips]
                o1 = out[(j * kinds + k) * owners + chips : (j * kinds + k + 1) * owners]
                keep_ref[t * chips : (t + 1) * chips, at] = jnp.where(first, o0, o1)
                send_ref[t * chips : (t + 1) * chips, at] = jnp.where(first, o1, o0).astype(
                    jnp.bfloat16
                )
            rows = slice(kind0 * owners, (kind0 + kinds) * owners)
            mine = log[j * kinds * owners : (j + 1) * kinds * owners]
            logs[rows, :] = jnp.where(lane[rows] == h, mine, logs[rows, :])

    for g in range(KVH):
        at = slice(g * HD, (g + 1) * HD)
        heads = [g * group + j for j in range(group)]
        spans, decodes = [], []
        for j in range(group):
            dev = 2 * g + j // per_dev
            col = slice((j % per_dev) * HD, (j % per_dev + 1) * HD)
            spans.append(q_ref[dev, 0:owners, col])
            decodes.append(q_ref[dev, owners : TYPES * owners, col])
        qs = jnp.concatenate(spans, axis=0)
        qd = jnp.concatenate(decodes, axis=0)
        out, log = soften(nt_dot(qs, pk_ref[:, at]), seen, pv_ref[:, at], group)
        place(out, log, heads, g, 0, 1)
        out, log = soften(nt_dot(qd, ck_ref[:, at]), live, cv_ref[:, at], group)
        place(out, log, heads, g, 1, STEPS)

    for t in range(TYPES):
        l0 = logs[t * owners : t * owners + chips, :]
        l1 = logs[t * owners + chips : (t + 1) * owners, :]
        rows = slice(t * chips, (t + 1) * chips)
        keep_log[rows, :] = jnp.where(first, l0, l1)
        parts = split3(jnp.where(first, l1, l0))
        for i in range(3):
            send_log[rows, i * HD : (i + 1) * HD] = parts[i]


def pair_kernel(me_ref, keep_ref, keep_log, got_ref, got_log, *rest):
    outs = rest[:-2]
    cut, cut_log = rest[-2:]
    chips = len(outs)
    width = D // SEGMENTS
    heads_seg = H // SEGMENTS
    chip = me_ref[0] // 2
    for t in range(TYPES):
        rows = slice(t * chips, (t + 1) * chips)
        la = keep_log[rows, :]
        lb = (
            got_log[rows, 0:HD].astype(jnp.float32)
            + got_log[rows, HD : 2 * HD].astype(jnp.float32)
            + got_log[rows, 2 * HD : 3 * HD].astype(jnp.float32)
        )
        top = jnp.maximum(la, lb)
        ea = jnp.exp(la - top)
        eb = jnp.exp(lb - top)
        total = ea + eb
        log = top + jnp.log(total)
        wa = ea / total
        wb = eb / total
        for s in range(SEGMENTS):
            base = t * chips * SEGMENTS + s
            for j in range(heads_seg):
                h = s * heads_seg + j
                at = slice(h * HD, (h + 1) * HD)
                both = keep_ref[rows, at] * wa[:, h : h + 1] + got_ref[rows, at].astype(
                    jnp.float32
                ) * wb[:, h : h + 1]
                cut[j, pl.ds(base, chips, stride=SEGMENTS), :] = both
            turned = log if s == 0 else pltpu.roll(log, HD - s * heads_seg, 1)
            cut_log[pl.ds(base, chips, stride=SEGMENTS), :] = turned
    lane = lax.broadcasted_iota(jnp.int32, (SEGMENTS, HD), 1)
    for k in range(chips):
        to = chip ^ k
        for t in range(TYPES):
            start = pl.multiple_of((t * chips + to) * SEGMENTS, SEGMENTS)
            rows = slice(t * SEGMENTS, (t + 1) * SEGMENTS)
            for j in range(heads_seg):
                outs[k][rows, j * HD : (j + 1) * HD] = cut[j, pl.ds(start, SEGMENTS), :].astype(
                    jnp.bfloat16
                )
            hi, mid, low = (
                v.astype(jnp.float32) for v in split3(cut_log[pl.ds(start, SEGMENTS), :])
            )
            packed = jnp.where(
                lane < heads_seg,
                hi,
                jnp.where(
                    lane < 2 * heads_seg,
                    pltpu.roll(mid, heads_seg, 1),
                    pltpu.roll(low, 2 * heads_seg, 1),
                ),
            )
            outs[k][rows, width:] = packed.astype(jnp.bfloat16)


def fresh_kernel(me_ref, q_ref, out_ref, log_ref, cache_ref, wide, own):
    devices = q_ref.shape[0]
    owners = devices
    chips = owners // 2
    group = H // KVH
    per_dev = group // 2
    cols = per_dev * HD
    me = me_ref[0]
    place = (me % 2) * chips + me // 2
    total = TYPES * owners
    for d in range(devices):
        wide[d] = q_ref[d].astype(jnp.float32)
    for d in range(devices):
        for t in range(TYPES):
            own[d, t : t + 1, :] = wide[d, pl.ds(t * owners + place, 1), :]
        cache_ref[:, d * HD : (d + 1) * HD] = own[d, 0:1, cols:].astype(jnp.bfloat16)
    key = lax.broadcasted_iota(jnp.int32, (SEGMENTS, total), 1)
    kind_k = key // owners
    within = key % owners
    owner_k = (within % chips) * 2 + within // chips
    kind_q = lax.broadcasted_iota(jnp.int32, (SEGMENTS, total), 0)
    span_bias = jnp.where((kind_k == 0) & (owner_k <= me), 0.0, neg_fill)
    step_bias = jnp.where(
        (kind_k >= 1) & (kind_k <= kind_q) & (owner_k == me), 0.0, neg_fill
    )
    bias = jnp.where(kind_q == 0, span_bias, step_bias)
    lane = lax.broadcasted_iota(jnp.int32, (SEGMENTS, HD), 1)
    for g in range(KVH):
        tiles = []
        for j in range(group):
            dev = 2 * g + j // per_dev
            col = slice((j % per_dev) * HD, (j % per_dev + 1) * HD)
            tiles.append(own[dev, :, col])
        q = jnp.concatenate(tiles, axis=0).astype(jnp.bfloat16)
        keys = q_ref[g, :, cols:]
        values = q_ref[KVH + g, :, cols:]
        out, log = soften(nt_dot(q, keys), bias, values, group)
        logs = jnp.zeros((SEGMENTS, HD), jnp.float32)
        for j in range(group):
            logs = jnp.where(lane == j, log[j * SEGMENTS : (j + 1) * SEGMENTS], logs)
        for t in range(TYPES):
            at = t * SEGMENTS + g
            log_ref[at : at + 1, :] = logs[t : t + 1]
            for j in range(group):
                out_ref[at : at + 1, j * HD : (j + 1) * HD] = out[
                    j * SEGMENTS + t : j * SEGMENTS + t + 1
                ]


def finish_kernel(*refs):
    fresh_ref, fresh_log = refs[:2]
    parts = refs[2:-3]
    span_ref, decode_ref, joined = refs[-3:]
    width = D // SEGMENTS
    heads_seg = H // SEGMENTS
    logs = [fresh_log[...]]
    for ref in parts:
        packed = ref[:, width:].astype(jnp.float32)
        logs.append(
            packed
            + pltpu.roll(packed, HD - heads_seg, 1)
            + pltpu.roll(packed, HD - 2 * heads_seg, 1)
        )
    top = logs[0]
    for log in logs[1:]:
        top = jnp.maximum(top, log)
    weights = [jnp.exp(log - top) for log in logs]
    total = weights[0]
    for w in weights[1:]:
        total = total + w
    weights = [w / total for w in weights]
    for j in range(heads_seg):
        at = slice(j * HD, (j + 1) * HD)
        out = fresh_ref[:, at] * weights[0][:, j : j + 1]
        for ref, w in zip(parts, weights[1:]):
            out = out + ref[:, at].astype(jnp.float32) * w[:, j : j + 1]
        joined[:, at] = out
    for s in range(SEGMENTS):
        cut = slice(s * width, (s + 1) * width)
        span_ref[:, cut] = joined[s : s + 1, :].astype(jnp.bfloat16)
        for t in range(STEPS):
            at = (t + 1) * SEGMENTS + s
            decode_ref[t : t + 1, cut] = joined[at : at + 1, :].astype(jnp.bfloat16)


def shards(
    span_rows, decode_rows, norm_gain, w_query, w_keyval, prefix_keys, prefix_values,
    span_offset, pool_keys, pool_values, row_blocks, context_lens,
):
    n = lax.axis_size("tensor")
    f32, bf16 = jnp.float32, jnp.bfloat16
    me = lax.axis_index("tensor").astype(jnp.int32).reshape(1)
    chips = n // 2
    rows_all = TYPES * n
    width = D // SEGMENTS
    cols = w_query.shape[1] + w_keyval.shape[1]
    unit = TYPES * SEGMENTS
    pk, pv = prefix_keys, prefix_values
    ck = pool_keys.reshape(-1, KVH * HD)
    cv = pool_values.reshape(-1, KVH * HD)

    def shape(dims, dtype):
        return jax.ShapeDtypeStruct(dims, dtype)

    normed = call(
        norm_kernel,
        shape((unit, width), bf16),
        [vmem(), vmem(), vmem()],
        [pltpu.VMEM((unit, width), f32), pltpu.VMEM((SEGMENTS, width), f32)],
        flops=unit * width * 8,
        name="norm",
    )(span_rows, decode_rows.reshape(STEPS, D), norm_gain.reshape(1, D))

    cos_tab, sin_tab = rotation_tables(HD // 2)
    cos_tab = jnp.concatenate([cos_tab, cos_tab], axis=1)
    sin_tab = jnp.concatenate([sin_tab, sin_tab], axis=1)
    cos, sin, live, seen = call(
        table_kernel,
        [
            shape((rows_all, HD), f32),
            shape((rows_all, HD), f32),
            shape((n, ck.shape[0]), f32),
            shape((8, pk.shape[0]), f32),
        ],
        [smem(), smem(), smem(), vmem(), vmem(), vmem()],
        [pltpu.VMEM((n, HD), jnp.int32)],
        flops=1 << 20,
        name="tables",
    )(me, span_offset, context_lens, row_blocks, cos_tab, sin_tab)

    gathered = lax.all_gather(normed, "tensor", axis=0, tiled=True)
    grid = (SEGMENTS,)
    fixed = lambda s: (0, 0)
    by_step = lambda s: (s, 0)
    projected = pl.pallas_call(
        project_kernel,
        grid=grid,
        out_shape=shape((rows_all, cols), bf16),
        in_specs=[
            smem(),
            vmem(),
            pl.BlockSpec((width, w_query.shape[1]), by_step),
            pl.BlockSpec((width, w_keyval.shape[1]), by_step),
            vmem(),
            vmem(),
        ],
        out_specs=pl.BlockSpec((rows_all, cols), fixed),
        scratch_shapes=[
            pltpu.VMEM((width // HD, n * unit, HD), f32),
            pltpu.VMEM((rows_all, cols), f32),
        ],
        compiler_params=pltpu.CompilerParams(vmem_limit_bytes=VMEM_LIMIT),
        cost_estimate=pl.CostEstimate(
            flops=2 * rows_all * D * cols, bytes_accessed=D * cols * 2, transcendentals=0
        ),
        name="project",
    )(me, gathered, w_query, w_keyval, cos, sin)

    everyone = lax.all_gather(projected, "tensor", axis=0, tiled=False)
    half = TYPES * chips
    keep, send, keep_log, send_log = call(
        attend_kernel,
        [
            shape((half, D), f32),
            shape((half, D), bf16),
            shape((half, HD), f32),
            shape((half, 3 * HD), bf16),
        ],
        [smem()] + [vmem()] * 7,
        [pltpu.VMEM((rows_all, HD), f32)],
        flops=4 * rows_all * D * ck.shape[0],
        name="attend",
    )(me, everyone, pk, pv, ck, cv, live, seen)

    swap = [(i, i ^ 1) for i in range(n)]
    got, got_log = (lax.ppermute(v, "tensor", swap) for v in (send, send_log))
    fresh, fresh_log, cache = call(
        fresh_kernel,
        [
            shape((unit, width), f32),
            shape((unit, HD), f32),
            shape((1, 2 * KVH * HD), bf16),
        ],
        [smem(), vmem()],
        [
            pltpu.VMEM((n, rows_all, cols), f32),
            pltpu.VMEM((n, SEGMENTS, cols), f32),
        ],
        flops=1 << 26,
        name="fresh",
    )(me, everyone)

    cuts = call(
        pair_kernel,
        [shape((unit, width + HD), bf16)] * chips,
        [smem()] + [vmem()] * 4,
        [
            pltpu.VMEM((width // HD, half * SEGMENTS, HD), f32),
            pltpu.VMEM((half * SEGMENTS, HD), f32),
        ],
        flops=half * D * 8,
        name="pair",
    )(me, keep, keep_log, got, got_log)
    parts = [cuts[0]] + [
        lax.ppermute(cuts[k], "tensor", [(i, i ^ (2 * k)) for i in range(n)])
        for k in range(1, chips)
    ]
    span_out, decode_out = call(
        finish_kernel,
        [shape((1, D), bf16), shape((STEPS, D), bf16)],
        [vmem()] * (2 + chips),
        [pltpu.VMEM((unit, width), f32)],
        flops=unit * width * 20,
        name="finish",
    )(fresh, fresh_log, *parts)
    return span_out, decode_out.reshape(STEPS, 1, D), cache


def fits(args, n):
    span_rows, decode_rows, w_query, w_keyval = args[0], args[1], args[3], args[4]
    return (
        span_rows.shape[0] == 1
        and decode_rows.shape[:2] == (STEPS, 1)
        and n == 2 * KVH
        and w_query.shape[1] * n == H * HD
        and w_keyval.shape[1] == HD
    )


def dispatch(*args):
    if fits(args, lax.axis_size("tensor")):
        return shards(*args)
    return generic_shards(*args)


def solution(mesh):
    in_specs = (
        P(("groups", "tensor"), None),
        P(None, ("groups", "tensor"), None),
        P(),
        P(None, "tensor"),
        P(None, "tensor"),
        P(("groups", "tensor"), None),
        P(("groups", "tensor"), None),
        P("groups"),
        P(("groups", "tensor"), None, None),
        P(("groups", "tensor"), None, None),
        P("groups", None),
        P("groups"),
    )
    out_specs = (
        P(("groups", "tensor"), None),
        P(None, ("groups", "tensor"), None),
        P(("groups", "tensor"), None),
    )
    return jax.shard_map(dispatch, mesh=mesh, in_specs=in_specs, out_specs=out_specs, check_vma=False)
```
